512 devices in a mesh: replica: 16 (over z, core), mp: 16 (over y, x_hi), refresh: 2 (over x_lo).
Axes of the slice: x: 4 (x_hi: 2, x_lo: 2; x = x_hi * 2 + x_lo), y: 8, z: 8, core: 2. Of those that a mesh axis runs over, the one named last changes fastest.
Arguments:
- grad_partial: bfloat16 [16, 2, 512, 8192], P('replica', 'refresh', 'mp'), may hold values from -63 to 63
- left_stats: float32 [2, 512, 8192], P('refresh', 'replica', 'mp'), may hold values from -4608 to 5120, as said below
- right_stats: float32 [2, 512, 8192], P('refresh', 'replica', 'mp'), may hold values from -4608 to 5120, as said below
- left_roots: float32 [2, 512, 8192], P('refresh', 'replica', 'mp'), may hold values from -1 to 1, as said below
- right_roots: float32 [2, 512, 8192], P('refresh', 'replica', 'mp'), may hold values from -1 to 1, as said below
- newton_counts: int32 [2, 16], replicated, may hold values from 1 to 4
- owner: int32 [2, 16], replicated, may hold values from 0 to 15, each once within a row
Outputs:
- update: float32 [2, 512, 8192], P('refresh', 'mp')
- new_left_stats: float32 [2, 512, 8192], P('refresh', 'replica', 'mp')
- new_right_stats: float32 [2, 512, 8192], P('refresh', 'replica', 'mp')
- new_left_roots: float32 [2, 512, 8192], P('refresh', 'replica', 'mp')
- new_right_roots: float32 [2, 512, 8192], P('refresh', 'replica', 'mp')
The draws below stay inside these ranges and needn't reach their ends.
Inputs may be any that keep to these rules, and one draw needn't show every extreme that they name: Each row of owner names every owner index once. `left_stats`: every 512 x 512 block is symmetric positive definite. `right_stats`: every 512 x 512 block is symmetric positive definite. `left_roots`: every 512 x 512 block is symmetric. `right_roots`: every 512 x 512 block is symmetric.
All inputs are finite; a program needn't handle non-finite values.
Results may differ from the reference program's by a relative error of at most 0.0003.
Values may be sent and summed in bfloat16 or wider, within the bound.
No kernel may reach another device: no remote copies, remote signals or barrier semaphores. Data moves between devices by JAX's collectives and lax.ppermute only.
A program may use at most 64 MiB of HBM per device.

```python
import math
import jax
import jax.numpy as jnp
from jax import lax

BLOCK = 512
MAX_NEWTON = 4
N_REPLICA = 16
N_MP = 16
N_REFRESH = 2


def draw_grad_partial(key, part):
    columns = BLOCK * N_MP
    first = jax.random.fold_in(key, 0)
    base = jnp.clip(jax.random.normal(first, (N_REPLICA, N_REFRESH, BLOCK, columns), jnp.float32), -6.0, 6.0)
    ramp = 1.0 + 2.0 * jnp.arange(N_MP, dtype=jnp.float32) / max(N_MP - 1, 1)
    column_scale = jnp.repeat(ramp, BLOCK)
    values = base
    return (values * column_scale * (4.0 / N_REPLICA)).astype(jnp.bfloat16)


def spd_blocks(key):
    normal = jnp.clip(jax.random.normal(key, (N_REFRESH, N_MP, BLOCK, BLOCK), jnp.float32), -6.0, 6.0)
    gram = jnp.einsum('fmik,fmjk->fmij', normal, normal) * 0.25 + BLOCK * 0.25 * jnp.eye(BLOCK, dtype=jnp.float32)
    return gram.transpose(0, 2, 1, 3).reshape(N_REFRESH, BLOCK, N_MP * BLOCK)


def near_identity(key):
    normal = jnp.clip(jax.random.normal(key, (N_REFRESH, N_MP, BLOCK, BLOCK), jnp.float32), -6.0, 6.0)
    symmetric = (normal + jnp.swapaxes(normal, -1, -2)) * (0.3 / math.sqrt(2.0 * BLOCK))
    roots = 0.25 * (jnp.eye(BLOCK, dtype=jnp.float32) + symmetric)
    return roots.transpose(0, 2, 1, 3).reshape(N_REFRESH, BLOCK, N_MP * BLOCK)


def draw_left_stats(key, part):
    return spd_blocks(jax.random.fold_in(key, 11))


def draw_right_stats(key, part):
    return spd_blocks(jax.random.fold_in(key, 12))


def draw_left_roots(key, part):
    return near_identity(jax.random.fold_in(key, 21))


def draw_right_roots(key, part):
    return near_identity(jax.random.fold_in(key, 22))


def with_ends(values, rng, low, high):
    extent = values.shape
    index_at = [jax.random.randint(jax.random.fold_in(rng, axis), (), 0, extent[axis]) for axis in range(len(extent))]
    values = values.at[tuple(index_at)].set(low)
    longest = extent.index(max(extent))
    index_at[longest] = (index_at[longest] + 1) % extent[longest]
    return values.at[tuple(index_at)].set(high)


def setup_inputs(seed: int = 0) -> dict:
    seeds = jax.random.split(jax.random.key(seed), 8)
    grad_partial = draw_grad_partial(jax.random.fold_in(seeds[7], 71), 0)
    left_stats = draw_left_stats(jax.random.fold_in(seeds[7], 71), 0)
    right_stats = draw_right_stats(jax.random.fold_in(seeds[7], 71), 0)
    left_roots = draw_left_roots(jax.random.fold_in(seeds[7], 71), 0)
    right_roots = draw_right_roots(jax.random.fold_in(seeds[7], 71), 0)
    newton_counts = with_ends(jax.random.randint(seeds[5], (N_REFRESH, N_MP), 1, MAX_NEWTON + 1), jax.random.fold_in(seeds[5], 1), 1, MAX_NEWTON).astype(jnp.int32)
    owner = jax.vmap(lambda own: jax.random.permutation(own, N_MP))(jax.random.split(seeds[6], N_REFRESH)).reshape((N_REFRESH, N_MP)).astype(jnp.int32)
    return dict(grad_partial=grad_partial, left_stats=left_stats, right_stats=right_stats, left_roots=left_roots, right_roots=right_roots, newton_counts=newton_counts, owner=owner)


decay = 0.9
graft_eps = 1e-06

def matmul(left, right):
    return jnp.einsum('nij,njk->nik', left, right, precision=lax.Precision.HIGHEST)

def by_owner(array):
    return array.reshape(N_REFRESH, BLOCK, N_MP, BLOCK).transpose(0, 2, 1, 3).reshape(N_REFRESH * N_MP, BLOCK, BLOCK)

def to_layout(array):
    return array.reshape(N_REFRESH, N_MP, BLOCK, BLOCK).transpose(0, 2, 1, 3).reshape(N_REFRESH, BLOCK, N_MP * BLOCK)

def newton(matrix, counts):
    eye = jnp.eye(BLOCK, dtype=jnp.float32)
    norm = jnp.sqrt(lax.optimization_barrier(jnp.sum(matrix * matrix, axis=(1, 2))))
    scale = 2.5 / norm
    iterate = (scale ** 0.25)[:, None, None] * eye
    coupled = scale[:, None, None] * matrix
    for step_index in range(MAX_NEWTON):
        factor = (5.0 * eye - coupled) * 0.25
        next_iterate = matmul(iterate, factor)
        next_coupled = matmul(matmul(matmul(matmul(coupled, factor), factor), factor), factor)
        live = (step_index < counts)[:, None, None]
        iterate = jnp.where(live, next_iterate, iterate)
        coupled = jnp.where(live, next_coupled, coupled)
    return iterate

def reference(grad_partial, left_stats, right_stats, left_roots, right_roots, newton_counts, owner):
    grad = lax.optimization_barrier(jnp.sum(grad_partial.astype(jnp.float32), axis=0))
    blocks = grad.reshape(N_REFRESH, BLOCK, N_MP, BLOCK).transpose(0, 2, 1, 3)
    inverse = jnp.argsort(owner, axis=1).astype(jnp.int32)
    owned = jnp.take_along_axis(blocks, inverse[:, :, None, None], axis=1).reshape(N_REFRESH * N_MP, BLOCK, BLOCK)
    counts = jnp.take_along_axis(newton_counts, inverse, axis=1).reshape(N_REFRESH * N_MP)
    flipped = jnp.transpose(owned, (0, 2, 1))
    new_left = decay * by_owner(left_stats) + (1.0 - decay) * matmul(owned, flipped)
    new_right = decay * by_owner(right_stats) + (1.0 - decay) * matmul(flipped, owned)
    direction = matmul(matmul(by_owner(left_roots), owned), by_owner(right_roots))
    grad_sq = jnp.sum(owned * owned)
    dir_sq = jnp.sum(direction * direction)
    scaled = direction * (jnp.sqrt(grad_sq) / jnp.sqrt(dir_sq + graft_eps))
    placed = jnp.take_along_axis(scaled.reshape(N_REFRESH, N_MP, BLOCK, BLOCK), owner.astype(jnp.int32)[:, :, None, None], axis=1)
    update = placed.transpose(0, 2, 1, 3).reshape(N_REFRESH, BLOCK, N_MP * BLOCK)
    left_root = newton(new_left, counts)
    right_root = newton(new_right, counts)
    return (update, to_layout(new_left), to_layout(new_right), to_layout(left_root), to_layout(right_root))
```

```python
import functools

import jax
import jax.numpy as jnp
from jax import lax
from jax.experimental import pallas as pl
from jax.experimental.pallas import tpu as pltpu
from jax.sharding import Mesh
from jax.sharding import PartitionSpec as P

MP = ("mp_0", "mp_1")
REPLICA = ("replica_0", "replica_1")

decay = 0.9
graft_eps = 1e-06

LANES = 128
HEAD = 8


def slot_owner(slot, part, n_long):
    return ((2 * n_long - part // 2 - slot // 2) % n_long) * 2 + slot % 2


def pair(a):
    high = a.astype(jnp.bfloat16)
    return high, (a - high.astype(jnp.float32)).astype(jnp.bfloat16)


def product(left, right, dims=((1,), (0,))):
    (lh, ll), (rh, rl) = left, right
    dot = functools.partial(
        lax.dot_general, dimension_numbers=(dims, ((), ())), preferred_element_type=jnp.float32
    )
    return dot(lh, rh) + (dot(lh, rl) + dot(ll, rh))


def mesh_place():
    owner_index = lax.axis_index("mp_0") * 2 + lax.axis_index("mp_1")
    replica_index = lax.axis_index("replica_0") * 2 + lax.axis_index("replica_1")
    return lax.axis_index("refresh"), owner_index, replica_index


def slot_columns(owner_ref, inverse_ref, group, part, slots):
    for block in range(slots):
        inverse_ref[owner_ref[group, block]] = block
    return [inverse_ref[slot_owner(slot, part, slots // 2)] for slot in range(slots)]


def bound_exponent(peak):
    return jnp.floor(jnp.log2(jnp.maximum(peak, 1e-30))) + 2.0


def coded(value, exponent):
    return jnp.round(value * jnp.exp2(23.0 - exponent)).astype(jnp.int32)


def encode(x, out_ref):
    rows = x.shape[0]
    exponent = bound_exponent(jnp.max(jnp.abs(x), axis=0, keepdims=True))
    q = coded(x, exponent)
    parts = [q[:, k * LANES : (k + 1) * LANES] for k in range(4)]
    for k in range(3):
        tail = (parts[3] >> (16 - 8 * k)) & 255
        out_ref[0:rows, k * LANES : (k + 1) * LANES] = (parts[k] << 8) | tail
    whole = exponent.astype(jnp.int32)
    out_ref[rows : rows + HEAD, :] = jnp.zeros((HEAD, 3 * LANES), jnp.int32)
    out_ref[rows : rows + 1, :] = whole[:, : 3 * LANES]
    out_ref[rows + 1 : rows + 2, :LANES] = whole[:, 3 * LANES :]


def decode(words, head, factor):
    parts = [words[:, k * LANES : (k + 1) * LANES] for k in range(3)]
    tail = (((parts[0] & 255) << 24) | ((parts[1] & 255) << 16) | ((parts[2] & 255) << 8)) >> 8
    exponents = [head[0:1, k * LANES : (k + 1) * LANES] for k in range(3)] + [head[1:2, :LANES]]
    whole = [p >> 8 for p in parts] + [tail]
    return [
        q.astype(jnp.float32) * (jnp.exp2(e.astype(jnp.float32) - 23.0) * factor)
        for q, e in zip(whole, exponents)
    ]


def order_kernel(owner_ref, rows_ref, out_ref, inverse_ref):
    group, part, _ = mesh_place()
    slots, _, order = out_ref.shape
    for slot, block in enumerate(slot_columns(owner_ref, inverse_ref, group, part, slots)):
        out_ref[slot] = rows_ref[:, pl.ds(pl.multiple_of(block * order, order), order)]


def sum_kernel(pieces_ref, out_ref):
    total = pieces_ref[0].astype(jnp.float32)
    for k in range(1, pieces_ref.shape[0]):
        total = total + pieces_ref[k].astype(jnp.float32)
    encode(total, out_ref)


def scalar_row(value):
    exponent = bound_exponent(value)
    return (
        jnp.broadcast_to(coded(value, exponent), (1, LANES)),
        jnp.broadcast_to(exponent.astype(jnp.int32), (1, LANES)),
    )


def total_sum(x):
    return jnp.sum(jnp.sum(x, axis=0, keepdims=True), axis=1, keepdims=True)


def direction_kernel(words_ref, roots_ref, grad_ref, coded_ref, norms_ref, hold_ref):
    order = grad_ref.shape[0]
    replica_index = mesh_place()[2]
    slots = words_ref.shape[0]
    rows = order // slots
    for k in range(slots):
        head = words_ref[k, rows : rows + HEAD, :]
        for c, part in enumerate(decode(words_ref[k, :rows, :], head, 1.0)):
            grad_ref[k * rows : (k + 1) * rows, c * LANES : (c + 1) * LANES] = part
    grad = grad_ref[...]
    half = product(pair(roots_ref[:, :order]), pair(grad))
    direction = product(pair(half), pair(roots_ref[:, order:]))
    hold_ref[...] = direction
    own = hold_ref[pl.ds(pl.multiple_of(replica_index * rows, rows), rows), :]
    encode(own, coded_ref)
    norms_ref[...] = jnp.zeros(norms_ref.shape, jnp.int32)
    for k, value in enumerate((total_sum(grad * grad), total_sum(direction * direction))):
        mantissa, exponent = scalar_row(value)
        for at in (coded_ref, norms_ref):
            row = rows + 2 + 2 * k if at is coded_ref else 4 + 2 * k - 2
            lane = 0 if at is coded_ref else LANES
            at[row : row + 1, lane : lane + LANES] = mantissa
            at[row + 1 : row + 2, lane : lane + LANES] = exponent


def newton_kernel(
    place_ref, owner_ref, counts_ref, grad_ref, stats_ref, mine_ref, theirs_ref,
    held_ref, factor_ref, high_ref, low_ref, rows_ref,
):
    group, owner_index, replica_index = mesh_place()
    order = grad_ref.shape[0]
    slots = counts_ref.shape[1]
    rows = order // slots
    count = jnp.int32(0)
    for block in range(slots):
        count = count + jnp.where(owner_ref[group, block] == owner_index, counts_ref[group, block], 0)
    parity = replica_index % 2
    grad = pair(grad_ref[...])

    def new_stats(term):
        held_ref[...] = decay * stats_ref[...] + (1.0 - decay) * term

    @pl.when(parity == 0)
    def _():
        new_stats(product(grad, grad, ((1,), (1,))))

    @pl.when(parity == 1)
    def _():
        new_stats(product(grad, grad, ((0,), (0,))))

    own = pl.multiple_of(replica_index * rows, rows)
    other = pl.multiple_of((replica_index + 1 - 2 * parity) * rows, rows)
    both = pl.multiple_of((replica_index - parity) * rows, 2 * rows)
    mine_ref[:rows, :] = held_ref[pl.ds(own, rows), :]
    theirs_ref[:rows, :] = held_ref[pl.ds(other, rows), :]
    full = held_ref[...]
    scale = 2.5 / jnp.sqrt(total_sum(full * full))
    held_ref[...] = scale * full
    start = jnp.sqrt(jnp.sqrt(scale))
    eye5 = jnp.where(
        lax.broadcasted_iota(jnp.int32, (order, order), 0)
        == lax.broadcasted_iota(jnp.int32, (order, order), 1),
        5.0,
        0.0,
    )

    def advance(step, carry):
        factor = (eye5 - held_ref[...]) * 0.25
        factor_ref[...] = factor
        split = pair(factor)

        @pl.when(step == 0)
        def _():
            rows_ref[...] = start * factor_ref[pl.ds(both, 2 * rows), :]

        @pl.when(step > 0)
        def _():
            rows_ref[...] = product(pair(rows_ref[...]), split)

        @pl.when(step < count - 1)
        def _():
            square = product(split, split)
            high_ref[...], low_ref[...] = pair(square)
            second = (high_ref[...], low_ref[...])
            fourth = product(second, second)
            high_ref[...], low_ref[...] = pair(fourth)
            held_ref[...] = product(pair(held_ref[...]), (high_ref[...], low_ref[...]))

        return carry

    lax.fori_loop(0, count, advance, jnp.int32(0))
    mine_ref[rows:, :] = rows_ref[pl.ds(pl.multiple_of(parity * rows, rows), rows), :]
    theirs_ref[rows:, :] = rows_ref[pl.ds(pl.multiple_of((1 - parity) * rows, rows), rows), :]


def finish_kernel(
    owner_ref, words_ref, mine_ref, theirs_ref,
    update_ref, left_ref, right_ref, left_root_ref, right_root_ref, inverse_ref,
):
    group, part, replica_index = mesh_place()
    slots = words_ref.shape[0]
    rows = words_ref.shape[1] - HEAD
    order = 4 * LANES

    def total(row):
        result = jnp.zeros((1, LANES), jnp.float32)
        for k in range(slots):
            for lane in (0, LANES):
                mantissa = words_ref[k, rows + row : rows + row + 1, lane : lane + LANES]
                exponent = words_ref[k, rows + row + 1 : rows + row + 2, lane : lane + LANES]
                result = result + mantissa.astype(jnp.float32) * jnp.exp2(
                    exponent.astype(jnp.float32) - 23.0
                )
        return result

    factor = jnp.sqrt(total(2)) / jnp.sqrt(total(4) + graft_eps)
    for slot, block in enumerate(slot_columns(owner_ref, inverse_ref, group, part, slots)):
        head = words_ref[slot, rows : rows + HEAD, :]
        base = pl.multiple_of(block * order, order)
        for c, piece in enumerate(decode(words_ref[slot, :rows, :], head, factor)):
            update_ref[:, pl.ds(pl.multiple_of(base + c * LANES, LANES), LANES)] = piece
    even = replica_index % 2 == 0
    mine, theirs = mine_ref[...], theirs_ref[...]
    left = jnp.where(even, mine, theirs)
    right = jnp.where(even, theirs, mine)
    left_ref[...], left_root_ref[...] = left[:rows], left[rows:]
    right_ref[...], right_root_ref[...] = right[:rows], right[rows:]


VMEM = pl.BlockSpec(memory_space=pltpu.VMEM)
SMEM = pl.BlockSpec(memory_space=pltpu.SMEM)


def local(grad_partial, left_stats, right_stats, left_roots, right_roots, newton_counts, owner):
    owners = lax.axis_size(MP)
    replicas = lax.axis_size(REPLICA)
    rows_part = grad_partial[0, 0]
    rows = rows_part.shape[0]
    order = rows_part.shape[1] // owners
    f32, i32 = jnp.float32, jnp.int32
    shape = jax.ShapeDtypeStruct

    inputs = jnp.concatenate([left_roots[0], right_roots[0], left_stats[0], right_stats[0]], axis=1)
    gathered = lax.all_gather(inputs, REPLICA, axis=0, tiled=True)

    ordered = pl.pallas_call(
        order_kernel,
        out_shape=shape((owners, rows, order), jnp.bfloat16),
        in_specs=[SMEM, VMEM],
        out_specs=VMEM,
        scratch_shapes=[pltpu.SMEM((owners,), i32)],
        name="order_blocks",
    )(owner, rows_part)
    arrived = lax.all_to_all(ordered, REPLICA, 0, 0, tiled=True)
    summed = pl.pallas_call(
        sum_kernel,
        out_shape=shape((rows + HEAD, 3 * LANES), i32),
        in_specs=[VMEM],
        out_specs=VMEM,
        name="sum_partials",
    )(arrived)

    there = [
        (slot * owners + part, part * owners + slot_owner(slot, part, owners // 2))
        for slot in range(replicas)
        for part in range(owners)
    ]
    back = [(b, a) for a, b in there]
    summed = lax.ppermute(summed, REPLICA + MP, there)
    words = lax.all_gather(summed, REPLICA, axis=0, tiled=False)

    grad, coded_rows, norms = pl.pallas_call(
        direction_kernel,
        grid=(1,),
        out_shape=(
            shape((order, order), f32),
            shape((rows + HEAD, 3 * LANES), i32),
            shape((HEAD, 3 * LANES), i32),
        ),
        in_specs=[VMEM, pl.BlockSpec((order, 2 * order), lambda i: (0, 0))],
        out_specs=(VMEM, VMEM, VMEM),
        scratch_shapes=[pltpu.VMEM((order, order), f32)],
        cost_estimate=pl.CostEstimate(
            flops=12 * order**3, bytes_accessed=20 * order**2, transcendentals=0
        ),
        name="direction",
    )(words, gathered)

    coded_rows = lax.ppermute(coded_rows, REPLICA + MP, back)
    crossed = [(2 * a + f, 2 * b + 1 - f) for a, b in back for f in (0, 1)]
    norms = lax.ppermute(norms, REPLICA + MP + ("refresh",), crossed)
    place = lax.axis_index(REPLICA) % 2

    mine, theirs = pl.pallas_call(
        newton_kernel,
        grid_spec=pltpu.PrefetchScalarGridSpec(
            num_scalar_prefetch=1,
            grid=(1,),
            in_specs=[
                SMEM,
                SMEM,
                VMEM,
                pl.BlockSpec((order, order), lambda i, parity: (0, 2 + parity[0])),
            ],
            out_specs=[VMEM, VMEM],
            scratch_shapes=[
                pltpu.VMEM((order, order), f32),
                pltpu.VMEM((order, order), f32),
                pltpu.VMEM((order, order), jnp.bfloat16),
                pltpu.VMEM((order, order), jnp.bfloat16),
                pltpu.VMEM((2 * rows, order), f32),
            ],
        ),
        out_shape=(shape((2 * rows, order), f32), shape((2 * rows, order), f32)),
        cost_estimate=pl.CostEstimate(
            flops=90 * order**3, bytes_accessed=8 * order**2, transcendentals=0
        ),
        name="newton",
    )(place.reshape(1), owner, newton_counts, grad, gathered)
    theirs = lax.ppermute(theirs, REPLICA, [(i, i ^ 1) for i in range(replicas)])

    payload = jnp.concatenate([coded_rows[:rows], coded_rows[rows:] + norms], axis=0)
    words = lax.all_gather(payload, REPLICA, axis=0, tiled=False)

    outs = pl.pallas_call(
        finish_kernel,
        out_shape=(shape((rows, owners * order), f32),) + (shape((rows, order), f32),) * 4,
        in_specs=[SMEM, VMEM, VMEM, VMEM],
        out_specs=(VMEM,) * 5,
        scratch_shapes=[pltpu.SMEM((owners,), i32)],
        name="finish",
    )(owner, words, mine, theirs)
    return tuple(out[None] for out in outs)


def solution(mesh):
    finer = Mesh(
        mesh.devices.reshape(8, 2, 8, 2, mesh.shape["refresh"]),
        ("replica_0", "replica_1", "mp_0", "mp_1", "refresh"),
    )
    in_specs = (
        P(REPLICA, "refresh", MP, None),
        P("refresh", REPLICA, MP),
        P("refresh", REPLICA, MP),
        P("refresh", REPLICA, MP),
        P("refresh", REPLICA, MP),
        P(),
        P(),
    )
    out_specs = (
        P("refresh", MP, None),
        P("refresh", REPLICA, MP),
        P("refresh", REPLICA, MP),
        P("refresh", REPLICA, MP),
        P("refresh", REPLICA, MP),
    )
    return jax.shard_map(local, mesh=finer, in_specs=in_specs, out_specs=out_specs, check_vma=False)
```

```python
import functools

import jax
import jax.numpy as jnp
from jax import lax
from jax.experimental import pallas as pl
from jax.experimental.pallas import tpu as pltpu
from jax.sharding import Mesh
from jax.sharding import PartitionSpec as P

MP = ("mp_0", "mp_1")
REPLICA = ("replica_0", "replica_1")

decay = 0.9
graft_eps = 1e-06

LANES = 128
HEAD = 8


def slot_owner(slot, part, n_long):
    return ((2 * (part // 2) + n_long // 2 - slot // 2 + n_long) % n_long) * 2 + slot % 2


def pair(a):
    high = a.astype(jnp.bfloat16)
    return high, (a - high.astype(jnp.float32)).astype(jnp.bfloat16)


def product(left, right, dims=((1,), (0,))):
    (lh, ll), (rh, rl) = left, right
    dot = functools.partial(
        lax.dot_general, dimension_numbers=(dims, ((), ())), preferred_element_type=jnp.float32
    )
    return dot(lh, rh) + (dot(lh, rl) + dot(ll, rh))


def mesh_place():
    owner_index = lax.axis_index("mp_0") * 2 + lax.axis_index("mp_1")
    replica_index = lax.axis_index("replica_0") * 2 + lax.axis_index("replica_1")
    return lax.axis_index("refresh"), owner_index, replica_index


def slot_columns(owner_ref, inverse_ref, group, part, slots):
    for block in range(slots):
        inverse_ref[owner_ref[group, block]] = block
    return [inverse_ref[slot_owner(slot, part, slots // 2)] for slot in range(slots)]


def bound_exponent(peak):
    return jnp.floor(jnp.log2(jnp.maximum(peak, 1e-30))) + 2.0


def coded(value, exponent):
    return jnp.round(value * jnp.exp2(23.0 - exponent)).astype(jnp.int32)


def encode(x, out_ref):
    rows = x.shape[0]
    exponent = bound_exponent(jnp.max(jnp.abs(x), axis=0, keepdims=True))
    q = coded(x, exponent)
    parts = [q[:, k * LANES : (k + 1) * LANES] for k in range(4)]
    for k in range(3):
        tail = (parts[3] >> (16 - 8 * k)) & 255
        out_ref[0:rows, k * LANES : (k + 1) * LANES] = (parts[k] << 8) | tail
    whole = exponent.astype(jnp.int32)
    out_ref[rows : rows + HEAD, :] = jnp.zeros((HEAD, 3 * LANES), jnp.int32)
    out_ref[rows : rows + 1, :] = whole[:, : 3 * LANES]
    out_ref[rows + 1 : rows + 2, :LANES] = whole[:, 3 * LANES :]


def decode(words, head, factor):
    parts = [words[:, k * LANES : (k + 1) * LANES] for k in range(3)]
    tail = (((parts[0] & 255) << 24) | ((parts[1] & 255) << 16) | ((parts[2] & 255) << 8)) >> 8
    exponents = [head[0:1, k * LANES : (k + 1) * LANES] for k in range(3)] + [head[1:2, :LANES]]
    whole = [p >> 8 for p in parts] + [tail]
    return [
        q.astype(jnp.float32) * (jnp.exp2(e.astype(jnp.float32) - 23.0) * factor)
        for q, e in zip(whole, exponents)
    ]


def encode_narrow(x, write):
    exponent = bound_exponent(jnp.max(jnp.abs(x), axis=0, keepdims=True)) - 1.0
    limit = 32767.0
    q = jnp.round(x * jnp.exp2(15.0 - exponent))
    q = jnp.clip(q, -limit, limit).astype(jnp.int32)
    half = x.shape[1] // 2
    write(0, (q[:, :half] << 16) | (q[:, half:] & 65535))
    whole = exponent.astype(jnp.int32)
    write(x.shape[0], whole[:, :half])
    write(x.shape[0] + 1, whole[:, half:])


def order_kernel(
    owner_ref, rows_ref, left_stats_ref, right_stats_ref, left_roots_ref, right_roots_ref,
    out_ref, inputs_ref, inverse_ref,
):
    group, part, _ = mesh_place()
    slots, _, order = out_ref.shape
    for k, ref in enumerate((left_roots_ref, right_roots_ref, left_stats_ref, right_stats_ref)):
        inputs_ref[:, k * order : (k + 1) * order] = ref[...]
    for slot, block in enumerate(slot_columns(owner_ref, inverse_ref, group, part, slots)):
        out_ref[slot] = rows_ref[:, pl.ds(pl.multiple_of(block * order, order), order)]


def sum_kernel(pieces_ref, out_ref):
    total = pieces_ref[0].astype(jnp.float32)
    for k in range(1, pieces_ref.shape[0]):
        total = total + pieces_ref[k].astype(jnp.float32)
    encode(total, out_ref)


def scalar_row(value):
    exponent = bound_exponent(value)
    return (
        jnp.broadcast_to(coded(value, exponent), (1, LANES)),
        jnp.broadcast_to(exponent.astype(jnp.int32), (1, LANES)),
    )


def total_sum(x):
    return jnp.sum(jnp.sum(x, axis=0, keepdims=True), axis=1, keepdims=True)


def direction_kernel(
    words_ref, inputs_ref, out_ref, coded_ref,
    grad_ref, left_ref, right_ref, hold_ref, left_sem, right_sem, grad_sem,
):
    order = grad_ref.shape[0]
    slots = words_ref.shape[0]
    rows = order // slots
    left_copy = pltpu.make_async_copy(inputs_ref.at[:, :order], left_ref, left_sem)
    right_copy = pltpu.make_async_copy(inputs_ref.at[:, order : 2 * order], right_ref, right_sem)
    left_copy.start()
    right_copy.start()
    for k in range(slots):
        head = words_ref[k, rows : rows + HEAD, :]
        for c, part in enumerate(decode(words_ref[k, :rows, :], head, 1.0)):
            grad_ref[k * rows : (k + 1) * rows, c * LANES : (c + 1) * LANES] = part
    grad_copy = pltpu.make_async_copy(grad_ref, out_ref, grad_sem)
    grad_copy.start()
    grad = grad_ref[...]
    left_copy.wait()
    half = product(pair(left_ref[...]), pair(grad))
    right_copy.wait()
    direction = product(pair(half), pair(right_ref[...]))
    hold_ref[...] = direction
    norms = [scalar_row(total_sum(x * x)) for x in (grad, direction)]
    for k in range(slots):

        def write(at, value):
            coded_ref[k, at : at + value.shape[0], :] = value

        encode_narrow(hold_ref[k * rows : (k + 1) * rows, :], write)
        for n, parts in enumerate(norms):
            write(rows + 2 + n, jnp.concatenate(parts, axis=1))
        write(rows + 4, jnp.zeros((HEAD - 4, 2 * LANES), jnp.int32))
    grad_copy.wait()


def totals_of(returned, rows):
    lines = returned[:, rows + 2 : rows + 4, :]
    exponent = lines[:, :, LANES:].astype(jnp.float32) - 23.0
    return jnp.sum(lines[:, :, :LANES].astype(jnp.float32) * jnp.exp2(exponent), axis=0)


def newton_kernel(
    owner_ref, counts_ref, grad_ref, inputs_ref, mine_ref, theirs_ref,
    stats_ref, held_ref, factor_ref, high_ref, low_ref, rows_ref, grad_sem, stats_sem,
):
    group, owner_index, replica_index = mesh_place()
    order = grad_ref.shape[0]
    grad_copy = pltpu.make_async_copy(grad_ref, factor_ref, grad_sem)
    grad_copy.start()
    slots = counts_ref.shape[1]
    rows = order // slots
    count = jnp.int32(0)
    for block in range(slots):
        count = count + jnp.where(owner_ref[group, block] == owner_index, counts_ref[group, block], 0)
    parity = replica_index % 2
    side = pl.ds(pl.multiple_of((2 + parity) * order, order), order)
    stats_copy = pltpu.make_async_copy(inputs_ref.at[:, side], stats_ref, stats_sem)
    stats_copy.start()
    grad_copy.wait()
    grad = pair(factor_ref[...])
    stats_copy.wait()

    def new_stats(term):
        held_ref[...] = decay * stats_ref[...] + (1.0 - decay) * term

    @pl.when(parity == 0)
    def _():
        new_stats(product(grad, grad, ((1,), (1,))))

    @pl.when(parity == 1)
    def _():
        new_stats(product(grad, grad, ((0,), (0,))))

    own = pl.multiple_of(replica_index * rows, rows)
    other = pl.multiple_of((replica_index + 1 - 2 * parity) * rows, rows)
    both = pl.multiple_of((replica_index - parity) * rows, 2 * rows)
    mine_ref[:rows, :] = held_ref[pl.ds(own, rows), :]
    theirs_ref[:rows, :] = held_ref[pl.ds(other, rows), :]
    full = held_ref[...]
    scale = 2.5 / jnp.sqrt(total_sum(full * full))
    held_ref[...] = scale * full
    start = jnp.sqrt(jnp.sqrt(scale))
    eye5 = jnp.where(
        lax.broadcasted_iota(jnp.int32, (order, order), 0)
        == lax.broadcasted_iota(jnp.int32, (order, order), 1),
        5.0,
        0.0,
    )

    def advance(step, carry):
        factor = (eye5 - held_ref[...]) * 0.25
        factor_ref[...] = factor
        split = pair(factor)

        @pl.when(step == 0)
        def _():
            rows_ref[...] = start * factor_ref[pl.ds(both, 2 * rows), :]

        @pl.when(step > 0)
        def _():
            rows_ref[...] = product(pair(rows_ref[...]), split)

        @pl.when(step < count - 1)
        def _():
            square = product(split, split)
            high_ref[...], low_ref[...] = pair(square)
            second = (high_ref[...], low_ref[...])
            fourth = product(second, second)
            high_ref[...], low_ref[...] = pair(fourth)
            held_ref[...] = product(pair(held_ref[...]), (high_ref[...], low_ref[...]))

        return carry

    lax.fori_loop(0, count, advance, jnp.int32(0))
    mine_ref[rows:, :] = rows_ref[pl.ds(pl.multiple_of(parity * rows, rows), rows), :]
    theirs_ref[rows:, :] = rows_ref[pl.ds(pl.multiple_of((1 - parity) * rows, rows), rows), :]


def finish_kernel(
    owner_ref, words_ref, totals_ref, others_ref, mine_ref, theirs_ref,
    update_ref, left_ref, right_ref, left_root_ref, right_root_ref,
):
    group, _, replica_index = mesh_place()
    slots = words_ref.shape[0]
    rows = words_ref.shape[1] - HEAD
    order = 4 * LANES
    totals = totals_ref[...] + others_ref[...]
    factor = jnp.sqrt(totals[0:1, :]) / jnp.sqrt(totals[1:2, :] + graft_eps)
    for block in range(slots):
        slot = owner_ref[group, block]
        for c in range(2):
            lanes = slice(c * LANES, (c + 1) * LANES)
            words = words_ref[slot, :rows, lanes]
            for h, q in enumerate((words >> 16, (words << 16) >> 16)):
                exponent = words_ref[slot, rows + h : rows + h + 1, lanes].astype(jnp.float32)
                base = block * order + (2 * h + c) * LANES
                update_ref[:, base : base + LANES] = q.astype(jnp.float32) * (
                    jnp.exp2(exponent - 15.0) * factor
                )
    even = replica_index % 2 == 0
    mine, theirs = mine_ref[...], theirs_ref[...]
    left = jnp.where(even, mine, theirs)
    right = jnp.where(even, theirs, mine)
    left_ref[...], left_root_ref[...] = left[:rows], left[rows:]
    right_ref[...], right_root_ref[...] = right[:rows], right[rows:]


VMEM = pl.BlockSpec(memory_space=pltpu.VMEM)
SMEM = pl.BlockSpec(memory_space=pltpu.SMEM)
ANY = pl.BlockSpec(memory_space=pl.ANY)


def on_chip(array):
    return pltpu.with_memory_space_constraint(array, pltpu.VMEM)


def local(grad_partial, left_stats, right_stats, left_roots, right_roots, newton_counts, owner):
    owners = lax.axis_size(MP)
    replicas = lax.axis_size(REPLICA)
    rows_part = grad_partial[0, 0]
    rows = rows_part.shape[0]
    order = rows_part.shape[1] // owners
    f32, i32 = jnp.float32, jnp.int32
    shape = jax.ShapeDtypeStruct

    ordered, inputs = pl.pallas_call(
        order_kernel,
        out_shape=(pltpu.VMEM((owners, rows, order), jnp.bfloat16), shape((rows, 4 * order), f32)),
        in_specs=[SMEM] + [VMEM] * 5,
        out_specs=(VMEM, VMEM),
        scratch_shapes=[pltpu.SMEM((owners,), i32)],
        name="order_blocks",
    )(owner, rows_part, left_stats[0], right_stats[0], left_roots[0], right_roots[0])
    gathered = lax.all_gather(inputs, REPLICA, axis=0, tiled=True)
    arrived = lax.all_to_all(ordered, REPLICA, 0, 0, tiled=True)
    summed = pl.pallas_call(
        sum_kernel,
        out_shape=pltpu.VMEM((rows + HEAD, 3 * LANES), i32),
        in_specs=[VMEM],
        out_specs=VMEM,
        name="sum_partials",
    )(on_chip(arrived))

    there = [
        (slot * owners + part, part * owners + slot_owner(slot, part, owners // 2))
        for slot in range(replicas)
        for part in range(owners)
    ]
    summed = lax.ppermute(summed, REPLICA + MP, there)
    words = lax.all_gather(summed, REPLICA, axis=0, tiled=False)

    grad, coded_blocks = pl.pallas_call(
        direction_kernel,
        out_shape=(
            shape((order, order), f32),
            shape((owners, rows + HEAD, 2 * LANES), i32),
        ),
        in_specs=[VMEM, ANY],
        out_specs=(ANY, VMEM),
        scratch_shapes=[pltpu.VMEM((order, order), f32)] * 4 + [pltpu.SemaphoreType.DMA] * 3,
        cost_estimate=pl.CostEstimate(
            flops=12 * order**3, bytes_accessed=20 * order**2, transcendentals=0
        ),
        name="direction",
    )(on_chip(words), gathered)
    returned = lax.all_to_all(coded_blocks, MP, 0, 0, tiled=True)

    mine, theirs = pl.pallas_call(
        newton_kernel,
        in_specs=[SMEM, SMEM, ANY, ANY],
        out_specs=[VMEM, VMEM],
        scratch_shapes=[
            pltpu.VMEM((order, order), f32),
            pltpu.VMEM((order, order), f32),
            pltpu.VMEM((order, order), f32),
            pltpu.VMEM((order, order), jnp.bfloat16),
            pltpu.VMEM((order, order), jnp.bfloat16),
            pltpu.VMEM((2 * rows, order), f32),
            pltpu.SemaphoreType.DMA,
            pltpu.SemaphoreType.DMA,
        ],
        out_shape=(pltpu.VMEM((2 * rows, order), f32), pltpu.VMEM((2 * rows, order), f32)),
        cost_estimate=pl.CostEstimate(
            flops=90 * order**3, bytes_accessed=8 * order**2, transcendentals=0
        ),
        name="newton",
    )(owner, newton_counts, grad, gathered)
    theirs = lax.ppermute(theirs, REPLICA, [(i, i ^ 1) for i in range(replicas)])

    totals = totals_of(returned, rows)
    others = lax.ppermute(totals, "refresh", [(0, 1), (1, 0)])

    outs = pl.pallas_call(
        finish_kernel,
        out_shape=(shape((rows, owners * order), f32),) + (shape((rows, order), f32),) * 4,
        in_specs=[SMEM] + [VMEM] * 5,
        out_specs=(VMEM,) * 5,
        name="finish",
    )(owner, on_chip(returned), on_chip(totals), on_chip(others), on_chip(mine), on_chip(theirs))
    return tuple(out[None] for out in outs)


def solution(mesh):
    finer = Mesh(
        mesh.devices.reshape(8, 2, 8, 2, mesh.shape["refresh"]),
        ("replica_0", "replica_1", "mp_0", "mp_1", "refresh"),
    )
    in_specs = (
        P(REPLICA, "refresh", MP, None),
        P("refresh", REPLICA, MP),
        P("refresh", REPLICA, MP),
        P("refresh", REPLICA, MP),
        P("refresh", REPLICA, MP),
        P(),
        P(),
    )
    out_specs = (
        P("refresh", MP, None),
        P("refresh", REPLICA, MP),
        P("refresh", REPLICA, MP),
        P("refresh", REPLICA, MP),
        P("refresh", REPLICA, MP),
    )
    return jax.shard_map(local, mesh=finer, in_specs=in_specs, out_specs=out_specs, check_vma=False)
```

```python
import functools

import jax
import jax.numpy as jnp
from jax import lax
from jax.experimental import pallas as pl
from jax.experimental.pallas import tpu as pltpu
from jax.sharding import Mesh
from jax.sharding import PartitionSpec as P

MP = ("mp_0", "mp_1")
REPLICA = ("replica_0", "replica_1")

decay = 0.9
graft_eps = 1e-06

LANES = 128
HEAD = 8


def slot_owner(slot, part, n_long):
    return ((2 * (part // 2) + n_long // 2 - slot // 2 + n_long) % n_long) * 2 + slot % 2


def pair(a):
    high = a.astype(jnp.bfloat16)
    return high, (a - high.astype(jnp.float32)).astype(jnp.bfloat16)


def product(left, right, dims=((1,), (0,))):
    (lh, ll), (rh, rl) = left, right
    dot = functools.partial(
        lax.dot_general, dimension_numbers=(dims, ((), ())), preferred_element_type=jnp.float32
    )
    return dot(lh, rh) + (dot(lh, rl) + dot(ll, rh))


def mesh_place():
    owner_index = lax.axis_index("mp_0") * 2 + lax.axis_index("mp_1")
    replica_index = lax.axis_index("replica_0") * 2 + lax.axis_index("replica_1")
    return lax.axis_index("refresh"), owner_index, replica_index


def slot_columns(owner_ref, inverse_ref, group, part, slots):
    for block in range(slots):
        inverse_ref[owner_ref[group, block]] = block
    return [inverse_ref[slot_owner(slot, part, slots // 2)] for slot in range(slots)]


def bound_exponent(peak):
    return jnp.floor(jnp.log2(jnp.maximum(peak, 1e-30))) + 2.0


def coded(value, exponent):
    return jnp.round(value * jnp.exp2(23.0 - exponent)).astype(jnp.int32)


def encode_narrow(x, write):
    exponent = bound_exponent(jnp.max(jnp.abs(x), axis=0, keepdims=True)) - 1.0
    limit = 32767.0
    q = jnp.round(x * jnp.exp2(15.0 - exponent))
    q = jnp.clip(q, -limit, limit).astype(jnp.int32)
    half = x.shape[1] // 2
    write(0, (q[:, :half] << 16) | (q[:, half:] & 65535))
    whole = exponent.astype(jnp.int32)
    write(x.shape[0], whole[:, :half])
    write(x.shape[0] + 1, whole[:, half:])


def decode_narrow(words, head, factor):
    for c in range(2):
        lanes = slice(c * LANES, (c + 1) * LANES)
        for h, q in enumerate((words[:, lanes] >> 16, (words[:, lanes] << 16) >> 16)):
            exponent = head[h : h + 1, lanes].astype(jnp.float32)
            yield 2 * h + c, q.astype(jnp.float32) * (jnp.exp2(exponent - 15.0) * factor)


def order_kernel(
    owner_ref, rows_ref, left_stats_ref, right_stats_ref, left_roots_ref, right_roots_ref,
    out_ref, inputs_ref, inverse_ref,
):
    group, part, _ = mesh_place()
    slots, _, order = out_ref.shape
    for k, ref in enumerate((left_roots_ref, right_roots_ref, left_stats_ref, right_stats_ref)):
        inputs_ref[:, k * order : (k + 1) * order] = ref[...]
    for slot, block in enumerate(slot_columns(owner_ref, inverse_ref, group, part, slots)):
        out_ref[slot] = rows_ref[:, pl.ds(pl.multiple_of(block * order, order), order)]


def sum_kernel(pieces_ref, out_ref):
    total = pieces_ref[0].astype(jnp.float32)
    for k in range(1, pieces_ref.shape[0]):
        total = total + pieces_ref[k].astype(jnp.float32)
    rows = total.shape[0]

    def write(at, value):
        out_ref[at : at + value.shape[0], :] = value

    encode_narrow(total, write)
    write(rows + 2, jnp.zeros((HEAD - 2, 2 * LANES), jnp.int32))


def scalar_row(value):
    exponent = bound_exponent(value)
    return (
        jnp.broadcast_to(coded(value, exponent), (1, LANES)),
        jnp.broadcast_to(exponent.astype(jnp.int32), (1, LANES)),
    )


def total_sum(x):
    return jnp.sum(jnp.sum(x, axis=0, keepdims=True), axis=1, keepdims=True)


def direction_kernel(
    words_ref, inputs_ref, out_ref, coded_ref,
    grad_ref, left_ref, right_ref, hold_ref, left_sem, right_sem, grad_sem,
):
    order = grad_ref.shape[0]
    slots = words_ref.shape[0]
    rows = order // slots
    left_copy = pltpu.make_async_copy(inputs_ref.at[:, :order], left_ref, left_sem)
    right_copy = pltpu.make_async_copy(inputs_ref.at[:, order : 2 * order], right_ref, right_sem)
    left_copy.start()
    right_copy.start()
    for k in range(slots):
        head = words_ref[k, rows : rows + HEAD, :]
        for c, part in decode_narrow(words_ref[k, :rows, :], head, 1.0):
            grad_ref[k * rows : (k + 1) * rows, c * LANES : (c + 1) * LANES] = part
    grad_copy = pltpu.make_async_copy(grad_ref, out_ref, grad_sem)
    grad_copy.start()
    grad = grad_ref[...]
    left_copy.wait()
    half = product(pair(left_ref[...]), pair(grad))
    right_copy.wait()
    direction = product(pair(half), pair(right_ref[...]))
    hold_ref[...] = direction
    norms = [scalar_row(total_sum(x * x)) for x in (grad, direction)]
    for k in range(slots):

        def write(at, value):
            coded_ref[k, at : at + value.shape[0], :] = value

        encode_narrow(hold_ref[k * rows : (k + 1) * rows, :], write)
        for n, parts in enumerate(norms):
            write(rows + 2 + n, jnp.concatenate(parts, axis=1))
        write(rows + 4, jnp.zeros((HEAD - 4, 2 * LANES), jnp.int32))
    grad_copy.wait()


def totals_of(returned, rows):
    lines = returned[:, rows + 2 : rows + 4, :]
    exponent = lines[:, :, LANES:].astype(jnp.float32) - 23.0
    return jnp.sum(lines[:, :, :LANES].astype(jnp.float32) * jnp.exp2(exponent), axis=0)


def newton_kernel(
    owner_ref, counts_ref, grad_ref, inputs_ref, mine_ref, theirs_ref,
    stats_ref, held_ref, factor_ref, high_ref, low_ref, rows_ref, grad_sem, stats_sem,
):
    group, owner_index, replica_index = mesh_place()
    order = grad_ref.shape[0]
    grad_copy = pltpu.make_async_copy(grad_ref, factor_ref, grad_sem)
    grad_copy.start()
    slots = counts_ref.shape[1]
    rows = order // slots
    count = jnp.int32(0)
    for block in range(slots):
        count = count + jnp.where(owner_ref[group, block] == owner_index, counts_ref[group, block], 0)
    parity = replica_index % 2
    side = pl.ds(pl.multiple_of((2 + parity) * order, order), order)
    stats_copy = pltpu.make_async_copy(inputs_ref.at[:, side], stats_ref, stats_sem)
    stats_copy.start()
    grad_copy.wait()
    grad = pair(factor_ref[...])
    stats_copy.wait()

    def new_stats(term):
        held_ref[...] = decay * stats_ref[...] + (1.0 - decay) * term

    @pl.when(parity == 0)
    def _():
        new_stats(product(grad, grad, ((1,), (1,))))

    @pl.when(parity == 1)
    def _():
        new_stats(product(grad, grad, ((0,), (0,))))

    own = pl.multiple_of(replica_index * rows, rows)
    other = pl.multiple_of((replica_index + 1 - 2 * parity) * rows, rows)
    both = pl.multiple_of((replica_index - parity) * rows, 2 * rows)
    mine_ref[:rows, :] = held_ref[pl.ds(own, rows), :]
    theirs_ref[:rows, :] = held_ref[pl.ds(other, rows), :]
    full = held_ref[...]
    scale = 2.5 / jnp.sqrt(total_sum(full * full))
    held_ref[...] = scale * full
    start = jnp.sqrt(jnp.sqrt(scale))
    eye5 = jnp.where(
        lax.broadcasted_iota(jnp.int32, (order, order), 0)
        == lax.broadcasted_iota(jnp.int32, (order, order), 1),
        5.0,
        0.0,
    )

    def advance(step, carry):
        factor = (eye5 - held_ref[...]) * 0.25
        factor_ref[...] = factor
        split = pair(factor)

        @pl.when(step == 0)
        def _():
            rows_ref[...] = start * factor_ref[pl.ds(both, 2 * rows), :]

        @pl.when(step > 0)
        def _():
            rows_ref[...] = product(pair(rows_ref[...]), split)

        @pl.when(step < count - 1)
        def _():
            square = product(split, split)
            high_ref[...], low_ref[...] = pair(square)
            second = (high_ref[...], low_ref[...])
            fourth = product(second, second)
            high_ref[...], low_ref[...] = pair(fourth)
            held_ref[...] = product(pair(held_ref[...]), (high_ref[...], low_ref[...]))

        return carry

    lax.fori_loop(0, count, advance, jnp.int32(0))
    mine_ref[rows:, :] = rows_ref[pl.ds(pl.multiple_of(parity * rows, rows), rows), :]
    theirs_ref[rows:, :] = rows_ref[pl.ds(pl.multiple_of((1 - parity) * rows, rows), rows), :]


def finish_kernel(
    owner_ref, words_ref, totals_ref, others_ref, mine_ref, theirs_ref,
    update_ref, left_ref, right_ref, left_root_ref, right_root_ref,
):
    group, _, replica_index = mesh_place()
    slots = words_ref.shape[0]
    rows = words_ref.shape[1] - HEAD
    order = 4 * LANES
    totals = totals_ref[...] + others_ref[...]
    factor = jnp.sqrt(totals[0:1, :]) / jnp.sqrt(totals[1:2, :] + graft_eps)
    for block in range(slots):
        slot = owner_ref[group, block]
        head = words_ref[slot, rows : rows + HEAD, :]
        for c, piece in decode_narrow(words_ref[slot, :rows, :], head, factor):
            base = block * order + c * LANES
            update_ref[:, base : base + LANES] = piece
    even = replica_index % 2 == 0
    mine, theirs = mine_ref[...], theirs_ref[...]
    left = jnp.where(even, mine, theirs)
    right = jnp.where(even, theirs, mine)
    left_ref[...], left_root_ref[...] = left[:rows], left[rows:]
    right_ref[...], right_root_ref[...] = right[:rows], right[rows:]


VMEM = pl.BlockSpec(memory_space=pltpu.VMEM)
SMEM = pl.BlockSpec(memory_space=pltpu.SMEM)
ANY = pl.BlockSpec(memory_space=pl.ANY)


def on_chip(array):
    return pltpu.with_memory_space_constraint(array, pltpu.VMEM)


def local(grad_partial, left_stats, right_stats, left_roots, right_roots, newton_counts, owner):
    owners = lax.axis_size(MP)
    replicas = lax.axis_size(REPLICA)
    rows_part = grad_partial[0, 0]
    rows = rows_part.shape[0]
    order = rows_part.shape[1] // owners
    f32, i32 = jnp.float32, jnp.int32
    shape = jax.ShapeDtypeStruct

    ordered, inputs = pl.pallas_call(
        order_kernel,
        out_shape=(pltpu.VMEM((owners, rows, order), jnp.bfloat16), shape((rows, 4 * order), f32)),
        in_specs=[SMEM] + [VMEM] * 5,
        out_specs=(VMEM, VMEM),
        scratch_shapes=[pltpu.SMEM((owners,), i32)],
        name="order_blocks",
    )(owner, rows_part, left_stats[0], right_stats[0], left_roots[0], right_roots[0])
    gathered = lax.all_gather(inputs, REPLICA, axis=0, tiled=True)
    arrived = lax.all_to_all(ordered, REPLICA, 0, 0, tiled=True)
    summed = pl.pallas_call(
        sum_kernel,
        out_shape=pltpu.VMEM((rows + HEAD, 2 * LANES), i32),
        in_specs=[VMEM],
        out_specs=VMEM,
        name="sum_partials",
    )(on_chip(arrived))

    there = [
        (slot * owners + part, part * owners + slot_owner(slot, part, owners // 2))
        for slot in range(replicas)
        for part in range(owners)
    ]
    summed = lax.ppermute(summed, REPLICA + MP, there)
    words = lax.all_gather(summed, REPLICA, axis=0, tiled=False)

    grad, coded_blocks = pl.pallas_call(
        direction_kernel,
        out_shape=(
            shape((order, order), f32),
            shape((owners, rows + HEAD, 2 * LANES), i32),
        ),
        in_specs=[VMEM, ANY],
        out_specs=(ANY, VMEM),
        scratch_shapes=[pltpu.VMEM((order, order), f32)] * 4 + [pltpu.SemaphoreType.DMA] * 3,
        cost_estimate=pl.CostEstimate(
            flops=12 * order**3, bytes_accessed=20 * order**2, transcendentals=0
        ),
        compiler_params=pltpu.CompilerParams(),
        name="direction",
    )(on_chip(words), gathered)
    returned = lax.all_to_all(coded_blocks, MP, 0, 0, tiled=True)

    mine, theirs = pl.pallas_call(
        newton_kernel,
        in_specs=[SMEM, SMEM, ANY, ANY],
        out_specs=[VMEM, VMEM],
        scratch_shapes=[
            pltpu.VMEM((order, order), f32),
            pltpu.VMEM((order, order), f32),
            pltpu.VMEM((order, order), f32),
            pltpu.VMEM((order, order), jnp.bfloat16),
            pltpu.VMEM((order, order), jnp.bfloat16),
            pltpu.VMEM((2 * rows, order), f32),
            pltpu.SemaphoreType.DMA,
            pltpu.SemaphoreType.DMA,
        ],
        out_shape=(pltpu.VMEM((2 * rows, order), f32), pltpu.VMEM((2 * rows, order), f32)),
        cost_estimate=pl.CostEstimate(
            flops=90 * order**3, bytes_accessed=8 * order**2, transcendentals=0
        ),
        name="newton",
    )(owner, newton_counts, grad, gathered)
    theirs = lax.ppermute(theirs, REPLICA, [(i, i ^ 1) for i in range(replicas)])

    totals = totals_of(returned, rows)
    others = lax.ppermute(totals, "refresh", [(0, 1), (1, 0)])

    outs = pl.pallas_call(
        finish_kernel,
        out_shape=(shape((rows, owners * order), f32),) + (shape((rows, order), f32),) * 4,
        in_specs=[SMEM] + [VMEM] * 5,
        out_specs=(VMEM,) * 5,
        name="finish",
    )(owner, on_chip(returned), on_chip(totals), on_chip(others), on_chip(mine), on_chip(theirs))
    return tuple(out[None] for out in outs)


def solution(mesh):
    finer = Mesh(
        mesh.devices.reshape(8, 2, 8, 2, mesh.shape["refresh"]),
        ("replica_0", "replica_1", "mp_0", "mp_1", "refresh"),
    )
    in_specs = (
        P(REPLICA, "refresh", MP, None),
        P("refresh", REPLICA, MP),
        P("refresh", REPLICA, MP),
        P("refresh", REPLICA, MP),
        P("refresh", REPLICA, MP),
        P(),
        P(),
    )
    out_specs = (
        P("refresh", MP, None),
        P("refresh", REPLICA, MP),
        P("refresh", REPLICA, MP),
        P("refresh", REPLICA, MP),
        P("refresh", REPLICA, MP),
    )
    return jax.shard_map(local, mesh=finer, in_specs=in_specs, out_specs=out_specs, check_vma=False)
```
